32 devices in a mesh: leaf: 2 (over core), row: 4 (over y, x), col: 4 (over z).
Axes of the slice: x: 2, y: 2, z: 4, core: 2. Of those that a mesh axis runs over, the one named last changes fastest.
Arguments:
- rhs_leaf: bfloat16 [2, 8, 64, 2048], P('leaf', None, None, 'col'), may hold values from -6 to 6
- dinv_leaf: bfloat16 [2, 8, 2048, 2048], P('leaf', None, 'row', 'col'), as said below
- panel_leaf: bfloat16 [2, 8, 1024, 2048], P('leaf', None, 'col', 'row'), may hold values from -0.0625 to 0.0625
- counts: int32 [2, 8], P('leaf'), may hold values from 256 to 2048, as said below
- row_index: int32 [2, 8, 1024], P('leaf'), may hold values from 0 to 4095, as said below
- rhs_root: bfloat16 [64, 4096], P(None, 'col'), may hold values from -6 to 6
- dinv_root: bfloat16 [4096, 4096], P(('leaf', 'row')), as said below
Outputs:
- y_leaf: bfloat16 [2, 8, 64, 2048], P('leaf', None, None, 'row')
- y_root: bfloat16 [64, 4096], P(None, ('leaf', 'row'))
The draws below stay inside these ranges and needn't reach their ends.
Inputs may be any that keep to these rules, and one draw needn't show every extreme that they name: `counts`: each subtree supernode has at least 256 columns; at least one supernode of every draw has all 2048. `row_index`: within one supernode the 1024 entries are distinct and increasing. `dinv_leaf`: each [2048, 2048] block is lower triangular with a nonzero diagonal. `dinv_root`: lower triangular with a nonzero diagonal.
All inputs are finite; a program needn't handle non-finite values.
Results may differ from the reference program's by a relative error of at most 0.0053.
Values may be sent and summed in bfloat16 or wider, within the bound.
No kernel may reach another device: no remote copies, remote signals or barrier semaphores. Data moves between devices by JAX's collectives and lax.ppermute only.
A program may use at most 64 MiB of HBM per device.

```python
import jax
import jax.numpy as jnp
from jax import lax

NRHS = 64
SA = 2048
RA = 1024
ST = 4096
KS = 8
GROUPS = 2
N_LEAF = 2


def lower_inverse(key, shape, order):
    first, second = jax.random.split(key)
    spread = jax.random.normal(first, shape, jnp.float32)
    diagonal = jax.random.uniform(second, shape[:-1], jnp.float32, 0.9, 1.3)
    lower = jnp.tril(spread * (0.6 / order ** 0.5), -1)
    eye = jnp.eye(order, dtype=jnp.float32)
    return lower + eye * diagonal[..., None]


def draw_dinv_leaf(key, part):
    return lower_inverse(jax.random.fold_in(key, 11), (GROUPS, KS, SA, SA), SA).astype(jnp.bfloat16)


def draw_dinv_root(key, part):
    return lower_inverse(jax.random.fold_in(key, 13), (ST, ST), ST).astype(jnp.bfloat16)


def draw_counts(key, part):
    first = jax.random.fold_in(key, 17)
    second = jax.random.fold_in(key, 19)
    values = jax.random.randint(first, (GROUPS * KS,), SA // 8, SA + 1)
    where = jax.random.randint(second, (), 0, GROUPS * KS)
    values = values.at[where].set(SA)
    return values.reshape(GROUPS, KS).astype(jnp.int32)


def draw_row_index(key, part):
    keys = jax.random.split(jax.random.fold_in(key, 23), GROUPS * KS)

    def pick(single):
        return jnp.sort(jax.random.permutation(single, ST)[:RA])
    chosen = jax.vmap(pick)(keys)
    return chosen.reshape(GROUPS, KS, RA).astype(jnp.int32)


def steps_of(rng, shape, cuts, smallest, high):
    def one(dim, parts):
        steps = jax.random.uniform(jax.random.fold_in(jax.random.fold_in(rng, 6), dim), (parts,), jnp.float32, smallest / len(cuts), high / len(cuts))
        return jnp.repeat(jnp.exp(steps), shape[dim] // parts).reshape((-1,) + (1,) * (len(shape) - dim - 1))

    gain = one(*cuts[0])
    for cut in cuts[1:]:
        gain = gain * one(*cut)
    return gain


def noise(own_key, shape, width, reach, cuts=(), kind=jnp.bfloat16):
    drawn = width * jax.random.normal(own_key, shape, jnp.float32)
    if cuts:
        drawn = drawn * steps_of(own_key, shape, cuts, -0.22, 0.18)
    return jnp.clip(drawn, -reach, reach).astype(kind)


def setup_inputs(seed: int = 0) -> dict:
    splits = jax.random.split(jax.random.key(seed), 8)
    return {
        "rhs_leaf": noise(splits[0], (GROUPS, KS, NRHS, SA), 1.0, 6.0, ((0, 2), (3, 4))),
        "dinv_leaf": draw_dinv_leaf(jax.random.fold_in(splits[7], 71), 0),
        "panel_leaf": noise(splits[2], (GROUPS, KS, RA, SA), (SA * N_LEAF * KS * RA // ST) ** -0.5, 0.0625, ((0, 2), (2, 4), (3, 4))),
        "counts": draw_counts(jax.random.fold_in(splits[7], 71), 0),
        "row_index": draw_row_index(jax.random.fold_in(splits[7], 71), 0),
        "rhs_root": noise(splits[5], (NRHS, ST), 1.0, 6.0, ((1, 4),)),
        "dinv_root": draw_dinv_root(jax.random.fold_in(splits[7], 71), 0),
    }


def reference(rhs_leaf, dinv_leaf, panel_leaf, counts, row_index, rhs_root, dinv_root):
    slots = lax.iota(jnp.int32, SA)
    flat_rhs = rhs_leaf.reshape(GROUPS * KS, NRHS, SA)
    flat_inv = dinv_leaf.reshape(GROUPS * KS, SA, SA)
    flat_panel = panel_leaf.reshape(GROUPS * KS, RA, SA)
    flat_count = counts.reshape(GROUPS * KS).astype(jnp.int32)
    flat_rows = row_index.reshape(GROUPS * KS, RA).astype(jnp.int32)

    def one_node(total, items):
        right, inverse, panel, count, targets = items
        live = slots[None, :] < count
        masked = jnp.where(live, right, jnp.zeros((), jnp.bfloat16))
        solved = jnp.dot(masked, inverse.T, preferred_element_type=jnp.float32)
        solved = jnp.where(live, solved, jnp.zeros((), jnp.float32)).astype(jnp.bfloat16)
        update = jnp.dot(solved, panel.T, preferred_element_type=jnp.float32)
        total = total.at[:, targets].add(update)
        return total, solved

    start = jnp.zeros((NRHS, ST), jnp.float32)
    gathered, solved_all = lax.scan(one_node, start, (flat_rhs, flat_inv, flat_panel, flat_count, flat_rows))
    reduced = (rhs_root.astype(jnp.float32) - gathered).astype(jnp.bfloat16)
    y_root = jnp.dot(reduced, dinv_root.T, preferred_element_type=jnp.float32).astype(jnp.bfloat16)
    return solved_all.reshape(GROUPS, KS, NRHS, SA), y_root
```

```python
import functools

import jax
import jax.numpy as jnp
from jax import lax
from jax.experimental import pallas as pl
from jax.experimental.pallas import tpu as pltpu
from jax.sharding import PartitionSpec as P

LANES = 128
VMEM = pltpu.VMEM
SMEM = pltpu.SMEM
NT = (((1,), (1,)), ((), ()))


def shift(value, axis, step):
    size = lax.axis_size(axis)
    pairs = [(i, (i + step) % size) for i in range(size)]
    return lax.ppermute(value, axis, pairs)


def leaf_kernel(cols, counts_ref, x_ref, d_ref, *out_refs):
    node = pl.program_id(0)
    col = lax.axis_index("col")
    share = x_ref.shape[1] // cols
    width = x_ref.shape[2]
    limit = counts_ref[0, node] - col * width
    rows = []
    for step in range(cols):
        start = pl.multiple_of(lax.rem(col + step, cols) * share, share)
        rows.append(x_ref[0, pl.ds(start, share), :])
    x = jnp.concatenate(rows, axis=0)
    slots = lax.broadcasted_iota(jnp.int32, x.shape, 1)
    x = jnp.where(slots < limit, x, jnp.zeros_like(x))
    product = lax.dot_general(x, d_ref[0], NT, preferred_element_type=jnp.float32)
    for step, ref in enumerate(out_refs):
        ref[0] = product[step * share:(step + 1) * share].astype(ref.dtype)


def leaf_partials(cols, counts, rhs, dinv):
    nodes, columns, width = rhs.shape
    height = dinv.shape[1]
    share = columns // cols
    out = [jax.ShapeDtypeStruct((nodes, share, height), jnp.bfloat16 if step else jnp.float32)
           for step in range(cols)]
    return pl.pallas_call(
        functools.partial(leaf_kernel, cols),
        grid=(nodes,),
        in_specs=[
            pl.BlockSpec(memory_space=SMEM),
            pl.BlockSpec((1, columns, width), lambda i: (i, 0, 0)),
            pl.BlockSpec((1, height, width), lambda i: (i, 0, 0)),
        ],
        out_specs=[pl.BlockSpec((1, share, height), lambda i: (i, 0, 0)) for _ in out],
        out_shape=out,
        name="leaf_partials",
        cost_estimate=pl.CostEstimate(
            flops=2 * nodes * columns * width * height,
            bytes_accessed=2 * dinv.size, transcendentals=0),
    )(counts, rhs, dinv)


def solve_kernel(counts_ref, own_ref, *refs):
    *got_refs, out_ref = refs
    nodes, share, height = own_ref.shape
    base = lax.axis_index("row") * height
    for node in range(nodes):
        total = own_ref[node]
        for ref in got_refs:
            total = total + ref[node].astype(jnp.float32)
        slots = lax.broadcasted_iota(jnp.int32, total.shape, 1) + base
        total = jnp.where(slots < counts_ref[0, node], total, jnp.zeros_like(total))
        out_ref[node] = total.astype(out_ref.dtype)


def whole_vmem(count):
    return [pl.BlockSpec(memory_space=VMEM) for _ in range(count)]


def solve_rows(counts, own, got):
    return pl.pallas_call(
        solve_kernel,
        in_specs=[pl.BlockSpec(memory_space=SMEM)] + whole_vmem(1 + len(got)),
        out_specs=pl.BlockSpec(memory_space=VMEM),
        out_shape=jax.ShapeDtypeStruct(own.shape, jnp.bfloat16),
        name="solve_rows",
    )(counts, own, *got)


def join_kernel(direction, *refs):
    *in_refs, out_ref = refs
    cols = len(in_refs)
    share = in_refs[0].shape[-2]
    col = lax.axis_index("col")
    for step, ref in enumerate(in_refs):
        start = pl.multiple_of(lax.rem(col + cols - step, cols) * share, share)
        if len(ref.shape) == 3:
            out_ref[:, pl.ds(start, share), :] = ref[...]
        else:
            out_ref[pl.ds(start, share), :] = ref[...]


def join_columns(pieces):
    shape = list(pieces[0].shape)
    shape[-2] *= len(pieces)
    return pl.pallas_call(
        functools.partial(join_kernel, 0),
        in_specs=whole_vmem(len(pieces)),
        out_specs=pl.BlockSpec(memory_space=VMEM),
        out_shape=jax.ShapeDtypeStruct(tuple(shape), pieces[0].dtype),
        name="join_columns",
    )(*pieces)


def gather_kernel(cols, leaves, starts_ref, code_ref, *refs):
    value_refs, out_refs, table_ref = refs[:cols], refs[cols:-1], refs[-1]
    nodes, share, panel = value_refs[0].shape
    tiles = code_ref.shape[0]
    part = tiles // leaves
    col = lax.axis_index("col")
    leaf = lax.axis_index("leaf") if leaves > 1 else 0
    for step, ref in enumerate(value_refs):
        start = pl.multiple_of(lax.rem(col + step, cols) * panel, panel)
        table_ref[:, :, pl.ds(start, panel)] = ref[...].astype(jnp.float32)
    lane = lax.broadcasted_iota(jnp.int32, (share, LANES), 1)
    for step, out_ref in enumerate(out_refs):
        block = lax.rem(leaf + step, leaves)

        @pl.loop(0, part)
        def _(index):
            tile = block * part + index
            total = jnp.zeros((share, LANES), jnp.float32)
            codes = code_ref[tile]
            for node in range(nodes):
                first = starts_ref[node, tile]
                base = pl.multiple_of((first // LANES) * LANES, LANES)
                low = table_ref[node, :, pl.ds(base, LANES)]
                high = table_ref[node, :, pl.ds(base + LANES, LANES)]
                window = jnp.where(lane >= lax.rem(first, LANES), low, high)
                code = jnp.broadcast_to(codes[node:node + 1], (share, LANES))
                picked = jnp.take_along_axis(
                    window, jnp.maximum(code, 0), axis=1, mode="promise_in_bounds")
                total = total + jnp.where(code >= 0, picked, 0.0)
            out_ref[:, pl.ds(pl.multiple_of(index * LANES, LANES), LANES)] = total.astype(
                out_ref.dtype)


def gather_updates(cols, leaves, starts, codes, values):
    nodes, share, panel = values[0].shape
    width = codes.shape[0] * LANES // leaves
    out = [jax.ShapeDtypeStruct((share, width), jnp.bfloat16 if step else jnp.float32)
           for step in range(leaves)]
    return pl.pallas_call(
        functools.partial(gather_kernel, cols, leaves),
        in_specs=[pl.BlockSpec(memory_space=SMEM)] + whole_vmem(1 + cols),
        out_specs=whole_vmem(leaves),
        out_shape=out,
        scratch_shapes=[VMEM((nodes, share, cols * panel + 2 * LANES), jnp.float32)],
        name="gather_updates",
    )(starts, codes, *values)


def reduce_kernel(cols, leaves, rhs_ref, own_ref, *refs):
    got_refs, rhs_refs, out_ref = refs[:-cols], refs[-cols:-1], refs[-1]
    share, width = own_ref.shape
    block = rhs_ref.shape[1]
    col = lax.axis_index("col")
    leaf = lax.axis_index("leaf")
    total = own_ref[...]
    for ref in got_refs:
        total = total + ref[...].astype(jnp.float32)
    mine = pl.ds(pl.multiple_of(col * share, share), share)
    count = max(1, width // block)
    span = min(width, block)
    for index in range(count):
        if width >= block:
            source, start = leaf * count + index, 0
        else:
            ratio = block // width
            source = leaf // ratio
            start = pl.multiple_of(lax.rem(leaf, ratio) * width, width)
        away = lax.rem(col + cols - source, cols)
        right = jnp.where(away == 0, rhs_ref[mine, pl.ds(start, span)].astype(jnp.float32), 0.0)
        for step, ref in enumerate(rhs_refs, 1):
            right = jnp.where(away == step, ref[:, pl.ds(start, span)].astype(jnp.float32), right)
        at = slice(index * span, (index + 1) * span)
        out_ref[:, at] = (right - total[:, at]).astype(out_ref.dtype)


def reduce_root(cols, leaves, rhs_root, own, got, rhs_got):
    return pl.pallas_call(
        functools.partial(reduce_kernel, cols, leaves),
        in_specs=whole_vmem(2 + len(got) + len(rhs_got)),
        out_specs=pl.BlockSpec(memory_space=VMEM),
        out_shape=jax.ShapeDtypeStruct(own.shape, jnp.bfloat16),
        name="reduce_root",
    )(rhs_root, own, *got, *rhs_got)


def sum_kernel(own_ref, *refs):
    *got_refs, out_ref, sent_ref = refs
    total = own_ref[...]
    for ref in got_refs:
        total = total + ref[...].astype(jnp.float32)
    out_ref[...] = total
    sent_ref[...] = total.astype(sent_ref.dtype)


def sum_leaves(own, got):
    return pl.pallas_call(
        sum_kernel,
        in_specs=whole_vmem(1 + len(got)),
        out_specs=whole_vmem(2),
        out_shape=[own, jax.ShapeDtypeStruct(own.shape, jnp.bfloat16)],
        name="sum_leaves",
    )(own, *got)


def send_rhs(cols, leaves, rhs_root):
    share = rhs_root.shape[0] // cols
    col = lax.axis_index("col")
    got = []
    for step in range(1, cols):
        start = lax.rem(col + step, cols) * share
        piece = lax.dynamic_slice_in_dim(rhs_root, start, share, 0)
        pairs = []
        for leaf in range(leaves):
            for source in range(leaf * cols // leaves, max(leaf * cols // leaves + 1, (leaf + 1) * cols // leaves)):
                pairs.append((leaf * cols + source, leaf * cols + (source + step) % cols))
        got.append(lax.ppermute(piece, ("leaf", "col"), pairs))
    return got


def index_tables(row_index, width):
    tiles = width // LANES
    rows = row_index.shape[1]
    high, low = row_index // LANES, row_index % LANES
    in_tile = high[:, None, :] == lax.iota(jnp.int32, tiles)[None, :, None]
    number = (lax.iota(jnp.int32, rows) % LANES).astype(jnp.bfloat16)
    is_lane = (low[:, :, None] == lax.iota(jnp.int32, LANES)).astype(jnp.bfloat16)
    left = jnp.stack([jnp.where(in_tile, number, 0), in_tile.astype(jnp.bfloat16)], 1)
    both = jnp.einsum("kntp,kpl->ntkl", left, is_lane, preferred_element_type=jnp.float32)
    codes = jnp.where(both[1] > 0.5, both[0], -1.0).astype(jnp.int32)
    before = high[:, None, :] < lax.iota(jnp.int32, tiles)[None, :, None]
    starts = jnp.sum(before.astype(jnp.int32), axis=2)
    return starts, codes


def local(rhs_leaf, dinv_leaf, panel_leaf, counts, row_index, rhs_root, dinv_root):
    cols, rows, leaves = (lax.axis_size(name) for name in ("col", "row", "leaf"))
    width = rhs_root.shape[1] * cols
    leaf = lax.axis_index("leaf")

    rhs_got = send_rhs(cols, leaves, rhs_root)
    partials = leaf_partials(cols, counts, rhs_leaf[0], dinv_leaf[0])
    got = [shift(partials[step], "col", step) for step in range(1, cols)]
    starts, codes = index_tables(row_index[0], width)
    solved = solve_rows(counts, partials[0], got)
    pieces = [solved] + [shift(solved, "col", step) for step in range(1, cols)]
    updates = []
    for step, piece in enumerate(pieces):
        update = jnp.einsum("kbi,kri->kbr", piece, panel_leaf[0], preferred_element_type=jnp.float32)
        if step:
            update = shift(update.astype(jnp.bfloat16), "col", cols - step)
        updates.append(update)
    y_leaf = join_columns(pieces)

    sums = gather_updates(cols, leaves, starts, codes, updates)
    sums_got = [shift(sums[step], "leaf", step) for step in range(1, leaves)]
    own, sent = sum_leaves(sums[0], sums_got)
    got = [shift(sent, "row", step) for step in range(1, rows)]
    reduced = reduce_root(cols, leaves, rhs_root, own, got, rhs_got)
    part = width // leaves
    total = 0.0
    for step in range(leaves):
        piece = shift(reduced, "leaf", step) if step else reduced
        block = lax.rem(leaf + leaves - step, leaves)
        inverse = lax.dynamic_slice_in_dim(dinv_root, block * part, part, 1)
        total = total + lax.dot_general(piece, inverse, NT, preferred_element_type=jnp.float32)
    mine = total.astype(jnp.bfloat16)
    y_root = join_columns([mine] + [shift(mine, "col", step) for step in range(1, cols)])
    return y_leaf[None], y_root


def solution(mesh):
    in_specs = (
        P("leaf", None, None, "col"),
        P("leaf", None, "row", "col"),
        P("leaf", None, "col", "row"),
        P("leaf", None),
        P("leaf", None, None),
        P(None, "col"),
        P(("leaf", "row"), None),
    )
    out_specs = (P("leaf", None, None, "row"), P(None, ("leaf", "row")))
    return jax.shard_map(local, mesh=mesh, in_specs=in_specs, out_specs=out_specs, check_vma=False)
```
